512 devices in a mesh: row: 64 (over y, z_hi, core), col: 8 (over z_lo, x).
Axes of the slice: x: 4, y: 8, z: 8 (z_hi: 4, z_lo: 2; z = z_hi * 2 + z_lo), core: 2. Of those that a mesh axis runs over, the one named last changes fastest.
Arguments:
- stiffness: bfloat16 [512, 768, 768], P(('row', 'col'))
- local_inverse: bfloat16 [512, 768, 768], P(('row', 'col'))
- averaging_basis: bfloat16 [512, 768, 64], P(('row', 'col')), may hold values from -0.4375 to 0.4375
- loads: bfloat16 [512, 768, 128], P(('row', 'col')), may hold values from -6 to 6
- start: float32 [98304, 128], P(('row', 'col')), may hold values from -6 to 6
- coarse_inverse: float32 [64, 8, 24, 12288], P(None, 'col', None, 'row')
- sizes: int32 [512], P(('row', 'col')), may hold values from 384 to 768, as said below
- dof_ids: int32 [512, 768], P(('row', 'col')), may hold values from 0 to 98303, as said below
- coarse_ids: int32 [512, 64], P(('row', 'col')), may hold values from 0 to 12287, as said below
Outputs:
- solution_field: float32 [98304, 128], P(('row', 'col'))
- residual: float32 [98304, 128], P(('row', 'col'))
The draws below stay inside these ranges and needn't reach their ends.
Inputs may be any that keep to these rules, and one draw needn't show every extreme that they name: `sizes`: the largest interface order, 768, occurs in every draw. `dof_ids`: subdomain s sits at row s // 8 and column s % 8; global interface dof g is owned by subdomain g // 192. The 768 slots of a subdomain hold distinct dofs, each owned by the subdomain itself or a subdomain at most one row and one column away; slots from sizes[s] on are not used. `coarse_ids`: coarse dof k is owned by subdomain k // 24. The 64 coarse dofs of a subdomain are distinct, each owned by the subdomain itself or a subdomain at most one row and one column away.
All inputs are finite; a program needn't handle non-finite values.
Results may differ from the reference program's by a relative error of at most 0.0064.
Values may be sent and summed in bfloat16 or wider, within the bound.
No kernel may reach another device: no remote copies, remote signals or barrier semaphores. Data moves between devices by JAX's collectives and lax.ppermute only.
A program may use at most 64 MiB of HBM per device.

```python
import jax
import jax.numpy as jnp
from jax import lax

NI = 768
OWN = 192
NP = 64
NCD = 24
COLS = 128
ITERS = 2
GROUPS = 64
MEMBERS = 8
SUBS = 512
NG = 98304
NCO = 12288


def square_blocks(key, spread):
    noise = jax.random.normal(key, (SUBS, NI, NI), jnp.float32)
    paired = (noise + jnp.swapaxes(noise, 1, 2)) * (spread / jnp.sqrt(2.0 * NI))
    diagonal = jax.random.uniform(jax.random.fold_in(key, 7), (SUBS, NI), jnp.float32, 0.6, 1.6)
    return paired + diagonal[:, :, None] * jnp.eye(NI, dtype=jnp.float32)[None]


def neighbour_ids(key, per_owner, keep):

    def one_subdomain(index):
        row_here = index // MEMBERS
        col_here = index % MEMBERS
        offsets = jnp.arange(3, dtype=jnp.int32) - 1
        row_list = row_here + offsets[:, None]
        col_list = col_here + offsets[None, :]
        inside = (row_list >= 0) & (row_list < GROUPS) & (col_list >= 0) & (col_list < MEMBERS)
        owner_index = row_list * MEMBERS + col_list
        candidates = (owner_index[:, :, None] * per_owner + jnp.arange(per_owner, dtype=jnp.int32)[None, None, :]).reshape(-1)
        valid = jnp.broadcast_to(inside[:, :, None], (3, 3, per_owner)).reshape(-1)
        shuffled = jax.random.permutation(jax.random.fold_in(key, index), 9 * per_owner).astype(jnp.int32)
        scores = jnp.where(valid, shuffled, shuffled - 9 * per_owner)
        best_scores, picked = lax.top_k(scores, keep)
        return candidates[picked]
    return jax.vmap(one_subdomain)(jnp.arange(SUBS, dtype=jnp.int32))


def draw_stiffness(key, part):
    return square_blocks(jax.random.fold_in(key, 21), 0.4).astype(jnp.bfloat16)


def draw_local_inverse(key, part):
    return square_blocks(jax.random.fold_in(key, 22), 0.5).astype(jnp.bfloat16)


def draw_coarse_inverse(key, part):
    noise = jax.random.normal(jax.random.fold_in(key, 31), (NCO, NCO), jnp.float32) / jnp.sqrt(1.0 * NCO)
    diagonal = jax.random.uniform(jax.random.fold_in(key, 32), (NCO,), jnp.float32, 0.5, 1.5)
    positions = jnp.arange(NCO, dtype=jnp.int32)
    matrix = noise.at[positions, positions].add(diagonal)
    return matrix.T.reshape(GROUPS, MEMBERS, NCD, NCO)


def draw_sizes(key, part):
    values = jax.random.randint(jax.random.fold_in(key, 41), (SUBS,), NI // 2, NI + 1)
    largest = jax.random.randint(jax.random.fold_in(key, 42), (), 0, SUBS)
    return values.at[largest].set(NI).astype(jnp.int32)


def draw_dof_ids(key, part):
    return neighbour_ids(jax.random.fold_in(key, 51), OWN, NI).astype(jnp.int32)


def draw_coarse_ids(key, part):
    return neighbour_ids(jax.random.fold_in(key, 52), NCD, NP).astype(jnp.int32)


def block_levels(key, dims, shards, low, high):
    def one(dim, shards_of):
        draws = jax.random.uniform(jax.random.fold_in(jax.random.fold_in(key, 6), dim), (shards_of,), jnp.float32, low / len(shards), high / len(shards))
        return jnp.repeat(jnp.exp(draws), dims[dim] // shards_of).reshape((-1,) + (1,) * (len(dims) - dim - 1))

    level = one(*shards[0])
    for cut in shards[1:]:
        level = level * one(*cut)
    return level


def bell_draw(own_key, dims, deviation, most, shards=(), kind=jnp.bfloat16):
    entries = deviation * jax.random.normal(own_key, dims, jnp.float32)
    if shards:
        entries = entries * block_levels(own_key, dims, shards, -0.22, 0.18)
    return jnp.clip(entries, -most, most).astype(kind)


def setup_inputs(seed: int = 0) -> dict:
    seeds = jax.random.split(jax.random.key(seed), 10)
    stiffness = draw_stiffness(jax.random.fold_in(seeds[9], 71), 0)
    local_inverse = draw_local_inverse(jax.random.fold_in(seeds[9], 71), 0)
    averaging_basis = bell_draw(seeds[2], (SUBS, NI, NP), (NI // 4) ** -0.5, 0.4375, ((0, 512),))
    loads = bell_draw(seeds[3], (SUBS, NI, COLS), 1.0, 6.0, ((0, 512),))
    start = bell_draw(seeds[4], (NG, COLS), 1.0, 6.0, ((0, 512),), jnp.float32)
    coarse_inverse = draw_coarse_inverse(jax.random.fold_in(seeds[9], 71), 0)
    sizes = draw_sizes(jax.random.fold_in(seeds[9], 71), 0)
    dof_ids = draw_dof_ids(jax.random.fold_in(seeds[9], 71), 0)
    coarse_ids = draw_coarse_ids(jax.random.fold_in(seeds[9], 71), 0)
    return dict(stiffness=stiffness, local_inverse=local_inverse, averaging_basis=averaging_basis, loads=loads, start=start, coarse_inverse=coarse_inverse, sizes=sizes, dof_ids=dof_ids, coarse_ids=coarse_ids)


def apply_each(matrices, vectors):
    return lax.map(lambda operands: jnp.dot(operands[0], operands[1], preferred_element_type=jnp.float32), (matrices, vectors))


def apply_transposed(matrices, vectors):
    return lax.map(lambda operands: jnp.dot(operands[0].T, operands[1], preferred_element_type=jnp.float32), (matrices, vectors))


def reference(stiffness, local_inverse, averaging_basis, loads, start, coarse_inverse, sizes, dof_ids, coarse_ids):
    slots = jnp.arange(NI, dtype=jnp.int32)
    live = slots[None, :] < sizes[:, None]
    live_float = live.astype(jnp.float32)
    target = jnp.where(live, dof_ids, NG).astype(jnp.int32)
    flat_target = target.reshape(-1)
    count = jax.ops.segment_sum(live_float.reshape(-1), flat_target, num_segments=NG + 1)
    weight = live_float / (count[dof_ids] + 1.0 - live_float)
    matrix = coarse_inverse.reshape(NCO, NCO)
    solution_field = start
    residual = start
    for repeat in range(ITERS):
        gathered = solution_field.astype(jnp.bfloat16)[dof_ids]
        local_iterate = jnp.where(live[:, :, None], gathered, jnp.zeros_like(gathered))
        image = apply_each(stiffness, local_iterate)
        terms = loads.astype(jnp.float32) - image
        residual = jax.ops.segment_sum(terms.reshape(-1, COLS), flat_target, num_segments=NG + 1)[:NG]
        scaled = (weight[:, :, None] * residual[dof_ids]).astype(jnp.bfloat16)
        local_part = apply_each(local_inverse, scaled)
        primal = apply_transposed(averaging_basis, scaled)
        coarse_rhs = jax.ops.segment_sum(primal.reshape(-1, COLS), coarse_ids.reshape(-1), num_segments=NCO)
        coarse_solution = jnp.dot(matrix.T, coarse_rhs, precision=lax.Precision.HIGHEST, preferred_element_type=jnp.float32).astype(jnp.bfloat16)
        correction = apply_each(averaging_basis, coarse_solution[coarse_ids])
        update = weight[:, :, None] * (local_part + correction)
        solution_field = solution_field + jax.ops.segment_sum(update.reshape(-1, COLS), flat_target, num_segments=NG + 1)[:NG]
    return solution_field, residual
```

```python
import jax
import jax.numpy as jnp
from jax import lax
from jax.experimental import pallas as pl
from jax.experimental.pallas import tpu as pltpu
from jax.sharding import PartitionSpec as P

ITERS = 2
LANES = 128
F32 = jnp.float32
BF16 = jnp.bfloat16
RES_A, RES_M, RES_B, RES_H = BF16, F32, F32, F32
COARSE_A, COARSE_M = BF16, F32
UPD_A, UPD_M, UPD_B = BF16, F32, F32
RHS_1, RHS_2, PART = BF16, BF16, F32


def dot(a, b):
    return jnp.dot(a, b, preferred_element_type=F32)


def call(kernel, outs, *args):
    return pl.pallas_call(
        kernel,
        out_shape=tuple(jax.ShapeDtypeStruct(s, d) for s, d in outs),
        compiler_params=pltpu.CompilerParams(vmem_limit_bytes=48 * 1024 * 1024),
    )(*args)


def window_positions(wanted, per_owner):
    members = lax.axis_size("col")
    owner = wanted // per_owner
    row_step = owner // members - lax.axis_index("row") + 1
    col_step = owner % members - lax.axis_index("col") + 1
    return row_step, col_step, wanted % per_owner


def pair(to_next, to_previous, axis):
    count = lax.axis_size(axis)
    from_previous = lax.ppermute(to_next, axis, [(i, i + 1) for i in range(count - 1)])
    from_next = lax.ppermute(to_previous, axis, [(i + 1, i) for i in range(count - 1)])
    return from_previous, from_next


def from_everyone(block, groups):
    copies = jnp.broadcast_to(block[None], (len(groups[0]), *block.shape))
    return lax.all_to_all(copies, "row", 0, 0, axis_index_groups=groups, tiled=True)


def wide(a):
    return a.astype(F32)


def sum_cols(left, middle, right):
    from_previous, from_next = pair(right, left, "col")
    return wide(middle) + wide(from_previous) + wide(from_next)


def sum_rows(summed, kind):
    third = summed.shape[0] // 3
    up, own, down = summed[:third], summed[third : 2 * third], summed[2 * third :]
    from_previous, from_next = pair(down.astype(kind), up.astype(kind), "row")
    return own + wide(from_previous) + wide(from_next)


def spread(owned):
    from_previous, from_next = pair(owned, owned, "row")
    column = jnp.concatenate([from_previous, owned, from_next], axis=0)
    left, right = pair(column, column, "col")
    return left, column, right


def prepare_kernel(pos_col, pos_row, coarse_col, coarse_row, out_col, basis, g, gt, cs, og, basis_t, counts):
    slots, window = g.shape
    own = window // 9
    g[...] = (pos_col[...] == lax.broadcasted_iota(jnp.int32, (slots, window), 1)).astype(F32).astype(BF16)
    gt[...] = (pos_row[...] == lax.broadcasted_iota(jnp.int32, (window, slots), 0)).astype(F32).astype(BF16)
    cs[...] = (coarse_row[...] == lax.broadcasted_iota(jnp.int32, cs.shape, 0)).astype(F32).astype(BF16)
    og[...] = (out_col[...] == lax.broadcasted_iota(jnp.int32, og.shape, 1)).astype(F32).astype(BF16)
    basis_t[...] = wide(basis[...]).T.astype(BF16)
    lane = lax.broadcasted_iota(jnp.int32, (slots, LANES), 1)
    counts[...] = jnp.zeros_like(counts)
    pos = jnp.broadcast_to(pos_col[...], (slots, LANES))
    for block in range(9):
        for half in range(-(-own // LANES)):
            hit = pos == lane + (block * own + half * LANES)
            row = block * 8 + half
            counts[row : row + 1, :] = jnp.sum(hit.astype(F32), axis=0, keepdims=True)


def panel_kernel(panel, high, low):
    turned = panel[...].T
    top = turned.astype(BF16)
    high[...] = top
    low[...] = (turned - top.astype(F32)).astype(BF16)


def picked(g, values):
    if values.dtype == BF16:
        return dot(g, values)
    high = values.astype(BF16)
    return dot(g, high) + dot(g, (values - wide(high)).astype(BF16))


def gathered(g, left, middle, right):
    third = left.shape[0]
    return (
        picked(g[:, :third], left) + picked(g[:, third : 2 * third], middle) + picked(g[:, 2 * third :], right)
    )


def scattered(gt, values, left, middle, right):
    third = left.shape[0]
    high = values.astype(BF16)
    low = (values - wide(high)).astype(BF16)
    for k, out in enumerate((left, middle, right)):
        rows = gt[k * third : (k + 1) * third]
        placed = dot(rows, high)
        if out.dtype == F32:
            placed = placed + dot(rows, low)
        out[...] = placed.astype(out.dtype)


def residual_kernel(win_l, win_m, win_r, g, gt, stiffness, loads, out_l, out_m, out_r):
    iterate = gathered(g, win_l[...], win_m[...], win_r[...]).astype(BF16)
    terms = wide(loads[...]) - dot(stiffness[...], iterate)
    scattered(gt, terms, out_l, out_m, out_r)


def weight_kernel(counts, pos_col, weight):
    slots = pos_col.shape[0]
    own = weight_own(counts)
    lane = lax.broadcasted_iota(jnp.int32, (slots, LANES), 1)
    pos = jnp.broadcast_to(pos_col[...], (slots, LANES))
    total = jnp.zeros((slots, LANES), F32)
    for block in range(9):
        for half in range(-(-own // LANES)):
            left = own - half * LANES
            hit = pos == lane + (block * own + half * LANES)
            if left < LANES:
                hit = hit & (lane < left)
            row = block * 8 + half
            total = total + jnp.where(hit, counts[row : row + 1, :], 0.0)
    shared = jnp.sum(total, axis=1, keepdims=True)
    live = (pos_col[...] >= 0).astype(F32)
    weight[...] = jnp.broadcast_to(live / (shared + 1.0 - live), weight.shape)


def weight_own(counts):
    return OWN_OF[counts.shape[0]]


OWN_OF = {}


def primal_kernel(win_l, win_m, win_r, g, weight, basis_t, cs, scaled, out_l, out_m, out_r):
    rows = gathered(g, win_l[...], win_m[...], win_r[...])
    values = (weight[...] * rows).astype(BF16)
    scaled[...] = values
    primal = dot(basis_t[...], values)
    scattered(cs, primal, out_l, out_m, out_r)


def local_kernel(local_inverse, scaled, out):
    out[...] = dot(local_inverse[...], scaled[...])


def fold_kernel(blocks, out):
    count = blocks.shape[0]
    third = blocks.shape[1] // 3
    for row in range(-1, count + 1):
        total = None
        for k in range(max(row - 1, 0), min(row + 1, count - 1) + 1):
            part = wide(blocks[k, (row - k + 1) * third : (row - k + 2) * third, :])
            total = part if total is None else total + part
        out[(row + 1) * third : (row + 2) * third, :] = total.astype(out.dtype)


def coarse_kernel(blocks, high, low, out, rhs):
    groups = blocks.shape[0]
    third = blocks.shape[1] // 10
    for y in range(groups):
        base = y * 8 * third
        rhs[base : base + 8 * third, :] = blocks[y, third : 9 * third, :]
        if y > 0:
            first = wide(blocks[y, third : 2 * third, :]) + wide(blocks[y - 1, 9 * third :, :])
            rhs[base : base + third, :] = first.astype(rhs.dtype)
        if y + 1 < groups:
            last = wide(blocks[y, 8 * third : 9 * third, :]) + wide(blocks[y + 1, :third, :])
            rhs[base + 7 * third : base + 8 * third, :] = last.astype(rhs.dtype)
    values = rhs[...]
    top = values.astype(BF16)
    part = dot(high[...], top) + dot(low[...], top)
    if rhs.dtype == F32:
        part = part + dot(high[...], (values - wide(top)).astype(BF16))
    part = part.astype(out.dtype)
    members = out.shape[0]
    for c in range(members):
        for step in range(3):
            owner = c + step - 1
            rows = slice(step * third, (step + 1) * third)
            if 0 <= owner < members:
                out[c, rows, :] = part[owner * third : (owner + 1) * third]
            else:
                out[c, rows, :] = jnp.zeros((third, LANES), out.dtype)


def update_kernel(sol_u, sol_m, sol_d, og, basis, weight, local_part, gt, out_l, out_m, out_r):
    third = sol_u.shape[0]
    coarse = (
        dot(og[:, :third], sol_u[...])
        + dot(og[:, third : 2 * third], sol_m[...])
        + dot(og[:, 2 * third :], sol_d[...])
    ).astype(BF16)
    update = weight[...] * (local_part[...] + dot(basis[...], coarse))
    scattered(gt, update, out_l, out_m, out_r)


def body(stiffness, local_inverse, averaging_basis, loads, start, coarse_inverse, sizes, dof_ids, coarse_ids):
    own = start.shape[0]
    per_coarse = coarse_inverse.shape[2]
    slots = dof_ids.shape[1]
    primals = coarse_ids.shape[1]
    rows = lax.axis_size("row")
    members = lax.axis_size("col")
    window, coarse_window = 9 * own, 9 * per_coarse
    inner = [[8 * y + k for k in range(8)] for y in range(rows // 8)]
    outer = [[8 * y + k for y in range(rows // 8)] for k in range(8)]
    halves = -(-own // LANES)
    OWN_OF[72] = own

    active = jnp.arange(slots, dtype=jnp.int32) < sizes[0]
    row_step, col_step, inside = window_positions(dof_ids[0], own)
    positions = jnp.where(active, (col_step * 3 + row_step) * own + inside, -1)
    row_step, col_step, inside = window_positions(coarse_ids[0], per_coarse)
    coarse_in = (col_step * 3 + row_step) * per_coarse + inside
    coarse_out = (row_step * 3 + col_step) * per_coarse + inside
    basis = averaging_basis[0]

    near = spread(start.astype(BF16))

    g, gt, cs, og, basis_t, counts = call(
        prepare_kernel,
        [
            ((slots, window), BF16),
            ((window, slots), BF16),
            ((coarse_window, primals), BF16),
            ((primals, coarse_window), BF16),
            ((primals, slots), BF16),
            ((72, LANES), F32),
        ],
        positions[:, None],
        positions[None, :],
        coarse_in[:, None],
        coarse_in[None, :],
        coarse_out[:, None],
        basis,
    )
    panel = coarse_inverse.reshape(-1, coarse_inverse.shape[3])
    high, low = call(panel_kernel, [(panel.shape[::-1], BF16)] * 2, panel)

    weight = None
    field = start
    residual = start
    for sweep in range(ITERS):
        third = 3 * own
        left, middle, right = call(
            residual_kernel,
            [((third, LANES), d) for d in (RES_A, RES_M, RES_A)],
            *near,
            g,
            gt,
            stiffness[0],
            loads[0],
        )
        if weight is None:
            def ride(part, column):
                parts = []
                for k in range(3):
                    parts.append(part[k * own : (k + 1) * own])
                    at = (3 * column + k) * 8
                    parts.append(counts[at : at + 8].astype(part.dtype))
                return jnp.concatenate(parts, axis=0)

            left, middle, right = ride(left, 0), ride(middle, 1), ride(right, 2)
        owned = sum_rows(sum_cols(left, middle, right), RES_B)
        residual = owned[:own]
        near = spread(owned.astype(RES_H))
        if weight is None:
            step = own + 8
            blocks = [n[k * step + own : (k + 1) * step] for n in near for k in range(3)]
            shared = jnp.concatenate([wide(b) for b in blocks], axis=0)
            near = tuple(
                jnp.concatenate([n[k * step : k * step + own] for k in range(3)], axis=0) for n in near
            )
            (weight,) = call(weight_kernel, [((slots, LANES), F32)], shared, positions[:, None])
        third = 3 * per_coarse
        scaled, left, middle, right = call(
            primal_kernel,
            [((slots, LANES), BF16)] + [((third, LANES), d) for d in (COARSE_A, COARSE_M, COARSE_A)],
            *near,
            g,
            weight,
            basis_t,
            cs,
        )
        (local_part,) = call(local_kernel, [((slots, LANES), F32)], local_inverse[0], scaled)
        mine = sum_cols(left, middle, right).astype(RHS_1)
        first = from_everyone(mine, inner)
        (folded,) = call(fold_kernel, [((10 * per_coarse, LANES), RHS_2)], first)
        second = from_everyone(folded, outer)
        parts, _ = call(
            coarse_kernel,
            [((members, third, LANES), PART), ((rows * per_coarse, LANES), RHS_2)],
            second,
            high,
            low,
        )
        parts = lax.all_to_all(parts, "col", 0, 0, tiled=True)
        totals = wide(parts).sum(axis=0).astype(BF16)
        above, below = pair(totals, totals, "row")
        third = 3 * own
        left, middle, right = call(
            update_kernel,
            [((third, LANES), d) for d in (UPD_A, UPD_M, UPD_A)],
            above,
            totals,
            below,
            og,
            basis,
            weight,
            local_part,
            gt,
        )
        field = field + sum_rows(sum_cols(left, middle, right), UPD_B)
        if sweep + 1 < ITERS:
            near = spread(field.astype(BF16))
    return field, residual


def solution(mesh):
    in_specs = (
        P(("row", "col"), None, None),
        P(("row", "col"), None, None),
        P(("row", "col"), None, None),
        P(("row", "col"), None, None),
        P(("row", "col"), None),
        P(None, "col", None, "row"),
        P(("row", "col")),
        P(("row", "col"), None),
        P(("row", "col"), None),
    )
    out_specs = (P(("row", "col"), None), P(("row", "col"), None))
    return jax.shard_map(body, mesh=mesh, in_specs=in_specs, out_specs=out_specs, check_vma=False)
```

```python
import jax
import jax.numpy as jnp
from jax import lax
from jax.experimental import pallas as pl
from jax.experimental.pallas import tpu as pltpu
from jax.sharding import PartitionSpec as P

ITERS = 2
LANES = 128
F32 = jnp.float32
BF16 = jnp.bfloat16
RES_A, RES_M, RES_B, RES_H = BF16, F32, F32, F32
COARSE_A, COARSE_M = BF16, F32
UPD_A, UPD_M, UPD_B = BF16, F32, F32
RHS_1, RHS_2, PART = BF16, BF16, F32


def dot(a, b):
    return jnp.dot(a, b, preferred_element_type=F32)


def call(kernel, outs, *args, scalar=None):
    specs = [pl.BlockSpec(memory_space=pltpu.VMEM)] * len(args)
    if scalar is not None:
        specs = [pl.BlockSpec(memory_space=pltpu.SMEM)] + specs
        args = (scalar, *args)
    return pl.pallas_call(
        kernel,
        out_shape=tuple(jax.ShapeDtypeStruct(s, d) for s, d in outs),
        in_specs=specs,
        compiler_params=pltpu.CompilerParams(vmem_limit_bytes=48 * 1024 * 1024),
    )(*args)


def window_positions(wanted, per_owner):
    members = lax.axis_size("col")
    owner = wanted // per_owner
    row_step = owner // members - lax.axis_index("row") + 1
    col_step = owner % members - lax.axis_index("col") + 1
    return row_step, col_step, wanted % per_owner


def pair(to_next, to_previous, axis):
    count = lax.axis_size(axis)
    from_previous = lax.ppermute(to_next, axis, [(i, i + 1) for i in range(count - 1)])
    from_next = lax.ppermute(to_previous, axis, [(i + 1, i) for i in range(count - 1)])
    return from_previous, from_next


def from_everyone(copies, groups):
    return lax.all_to_all(copies, "row", 0, 0, axis_index_groups=groups, tiled=True)


def wide(a):
    return a.astype(F32)


def spread(column):
    from_previous, from_next = pair(column, column, "row")
    return from_previous, column, from_next


def shared_by_columns(column, up, middle, down):
    from_previous, from_next = pair(down, up, "row")
    members = lax.axis_size("col")
    third = middle.shape[0] // 3
    summed, sent = call(
        send_kernel,
        [(middle.shape, F32), ((members, 2 * third, LANES), BF16)],
        from_previous,
        middle,
        from_next,
        scalar=column,
    )
    got = lax.all_to_all(sent, "col", 0, 0, tiled=True)
    (assembled,) = call(receive_kernel, [(middle.shape, F32)], got, summed, scalar=column)
    return assembled


def owned_sum(up, middle, down):
    from_previous, from_next = pair(down, up, "row")
    summed = wide(middle) + wide(from_previous) + wide(from_next)
    third = summed.shape[0] // 3
    left, own, right = summed[:third], summed[third : 2 * third], summed[2 * third :]
    from_previous, from_next = pair(right.astype(UPD_B), left.astype(UPD_B), "col")
    return own + wide(from_previous) + wide(from_next)


def nth(c, step, members):
    return lax.rem(c + step + members, members)


def send_kernel(column, from_previous, middle, from_next, summed, sent):
    third = middle.shape[0] // 3
    members = sent.shape[0]
    c = column[0]
    total = wide(from_previous[...]) + wide(middle[...]) + wide(from_next[...])
    summed[...] = total
    left, own, right = (total[k * third : (k + 1) * third].astype(BF16) for k in range(3))
    sent[nth(c, 1, members), :third, :] = own
    sent[nth(c, 1, members), third:, :] = right
    sent[nth(c, 2, members), :third, :] = right
    sent[nth(c, -1, members), :third, :] = own
    sent[nth(c, -1, members), third:, :] = left
    sent[nth(c, -2, members), :third, :] = left


def receive_kernel(column, got, summed, out):
    third = summed.shape[0] // 3
    members = got.shape[0]
    c = column[0]

    def part(step, rows):
        there = (c + step >= 0) & (c + step < members)
        return jnp.where(there, wide(got[nth(c, step, members), rows, :]), 0.0)

    first, second = slice(0, third), slice(third, 2 * third)
    out[:third] = summed[:third] + part(-1, first) + part(-2, first)
    out[third : 2 * third] = summed[third : 2 * third] + part(-1, second) + part(1, second)
    out[2 * third :] = summed[2 * third :] + part(1, first) + part(2, first)


def coarse_receive_kernel(column, got, middle, out):
    members = got.shape[0]
    c = column[0]
    total = wide(middle[...])
    for step in (-1, 1):
        there = (c + step >= 0) & (c + step < members)
        total = total + jnp.where(there, wide(got[nth(c, step, members)]), 0.0)
    total = total.astype(out.dtype)
    for k in range(out.shape[0]):
        out[k] = total


def prepare_kernel(pos_col, pos_row, coarse_col, coarse_row, out_col, basis, g, gt, cs, og, basis_t, counts):
    slots, window = g.shape
    own = window // 9
    g[...] = (pos_col[...] == lax.broadcasted_iota(jnp.int32, (slots, window), 1)).astype(F32).astype(BF16)
    gt[...] = (pos_row[...] == lax.broadcasted_iota(jnp.int32, (window, slots), 0)).astype(F32).astype(BF16)
    cs[...] = (coarse_row[...] == lax.broadcasted_iota(jnp.int32, cs.shape, 0)).astype(F32).astype(BF16)
    og[...] = (out_col[...] == lax.broadcasted_iota(jnp.int32, og.shape, 1)).astype(F32).astype(BF16)
    basis_t[...] = wide(basis[...]).T.astype(BF16)
    lane = lax.broadcasted_iota(jnp.int32, (slots, LANES), 1)
    counts[...] = jnp.zeros_like(counts)
    pos = jnp.broadcast_to(pos_col[...], (slots, LANES))
    for block in range(9):
        for half in range(-(-own // LANES)):
            hit = pos == lane + (block * own + half * LANES)
            row = block * 8 + half
            counts[row : row + 1, :] = jnp.sum(hit.astype(F32), axis=0, keepdims=True)


def panel_kernel(panel, high, low):
    turned = panel[...].T
    top = turned.astype(BF16)
    high[...] = top
    low[...] = (turned - top.astype(F32)).astype(BF16)


def picked(g, values):
    if values.dtype == BF16:
        return dot(g, values)
    high = values.astype(BF16)
    return dot(g, high) + dot(g, (values - wide(high)).astype(BF16))


def gathered(g, left, middle, right):
    third = left.shape[0]
    return (
        picked(g[:, :third], left) + picked(g[:, third : 2 * third], middle) + picked(g[:, 2 * third :], right)
    )


def scattered(gt, values, left, middle, right):
    third = left.shape[0]
    high = values.astype(BF16)
    low = (values - wide(high)).astype(BF16)
    for k, out in enumerate((left, middle, right)):
        rows = gt[k * third : (k + 1) * third]
        placed = dot(rows, high)
        if out.dtype == F32:
            placed = placed + dot(rows, low)
        out[...] = placed.astype(out.dtype)


def residual_kernel(win_l, win_m, win_r, g, gt, stiffness, loads, out_l, out_m, out_r):
    iterate = gathered(g, win_l[...], win_m[...], win_r[...]).astype(BF16)
    terms = wide(loads[...]) - dot(stiffness[...], iterate)
    scattered(gt, terms, out_l, out_m, out_r)


def weight_kernel(counts, pos_col, weight):
    slots = pos_col.shape[0]
    own = weight_own(counts)
    lane = lax.broadcasted_iota(jnp.int32, (slots, LANES), 1)
    pos = jnp.broadcast_to(pos_col[...], (slots, LANES))
    total = jnp.zeros((slots, LANES), F32)
    for block in range(9):
        for half in range(-(-own // LANES)):
            left = own - half * LANES
            hit = pos == lane + (block * own + half * LANES)
            if left < LANES:
                hit = hit & (lane < left)
            row = block * 8 + half
            total = total + jnp.where(hit, counts[row : row + 1, :], 0.0)
    shared = jnp.sum(total, axis=1, keepdims=True)
    live = (pos_col[...] >= 0).astype(F32)
    weight[...] = jnp.broadcast_to(live / (shared + 1.0 - live), weight.shape)


def weight_own(counts):
    return OWN_OF[counts.shape[0]]


OWN_OF = {}


def primal_kernel(column, up, middle, down, g, weight, basis_t, cs, scaled, sent, kept):
    rows = gathered(g, up[...], middle[...], down[...])
    values = (weight[...] * rows).astype(BF16)
    scaled[...] = values
    primal = dot(basis_t[...], values)
    third = kept.shape[0]
    members = sent.shape[0]
    c = column[0]
    high = primal.astype(BF16)
    low = (primal - wide(high)).astype(BF16)
    sent[nth(c, -1, members)] = dot(cs[:third], high).astype(sent.dtype)
    sent[nth(c, 1, members)] = dot(cs[2 * third :], high).astype(sent.dtype)
    rows = cs[third : 2 * third]
    kept[...] = dot(rows, high) + dot(rows, low)


def local_kernel(local_inverse, scaled, out):
    out[...] = dot(local_inverse[...], scaled[...])


def fold_kernel(blocks, out):
    count = blocks.shape[0]
    third = blocks.shape[1] // 3
    for row in range(-1, count + 1):
        total = None
        for k in range(max(row - 1, 0), min(row + 1, count - 1) + 1):
            part = wide(blocks[k, (row - k + 1) * third : (row - k + 2) * third, :])
            total = part if total is None else total + part
        total = total.astype(out.dtype)
        for copy in range(out.shape[0]):
            out[copy, (row + 1) * third : (row + 2) * third, :] = total


def coarse_kernel(blocks, high, low, out, rhs):
    groups = blocks.shape[0]
    third = blocks.shape[1] // 10
    for y in range(groups):
        base = y * 8 * third
        rhs[base : base + 8 * third, :] = blocks[y, third : 9 * third, :]
        if y > 0:
            first = wide(blocks[y, third : 2 * third, :]) + wide(blocks[y - 1, 9 * third :, :])
            rhs[base : base + third, :] = first.astype(rhs.dtype)
        if y + 1 < groups:
            last = wide(blocks[y, 8 * third : 9 * third, :]) + wide(blocks[y + 1, :third, :])
            rhs[base + 7 * third : base + 8 * third, :] = last.astype(rhs.dtype)
    values = rhs[...]
    top = values.astype(BF16)
    part = dot(high[...], top) + dot(low[...], top)
    if rhs.dtype == F32:
        part = part + dot(high[...], (values - wide(top)).astype(BF16))
    part = part.astype(out.dtype)
    members = out.shape[0]
    for c in range(members):
        for step in range(3):
            owner = c + step - 1
            rows = slice(step * third, (step + 1) * third)
            if 0 <= owner < members:
                out[c, rows, :] = part[owner * third : (owner + 1) * third]
            else:
                out[c, rows, :] = jnp.zeros((third, LANES), out.dtype)


def update_kernel(sol_u, sol_m, sol_d, og, basis, weight, local_part, gt, out_l, out_m, out_r):
    third = sol_u.shape[0]
    coarse = (
        dot(og[:, :third], sol_u[...])
        + dot(og[:, third : 2 * third], sol_m[...])
        + dot(og[:, 2 * third :], sol_d[...])
    ).astype(BF16)
    update = weight[...] * (local_part[...] + dot(basis[...], coarse))
    scattered(gt, update, out_l, out_m, out_r)


def body(stiffness, local_inverse, averaging_basis, loads, start, coarse_inverse, sizes, dof_ids, coarse_ids):
    own = start.shape[0]
    per_coarse = coarse_inverse.shape[2]
    slots = dof_ids.shape[1]
    primals = coarse_ids.shape[1]
    rows = lax.axis_size("row")
    members = lax.axis_size("col")
    window, coarse_window = 9 * own, 9 * per_coarse
    inner = [[8 * y + k for k in range(8)] for y in range(rows // 8)]
    outer = [[8 * y + k for y in range(rows // 8)] for k in range(8)]
    halves = -(-own // LANES)
    OWN_OF[72] = own

    column = lax.axis_index("col").astype(jnp.int32).reshape(1)

    active = jnp.arange(slots, dtype=jnp.int32) < sizes[0]
    row_step, col_step, inside = window_positions(dof_ids[0], own)
    positions = jnp.where(active, (row_step * 3 + col_step) * own + inside, -1)
    row_step, col_step, inside = window_positions(coarse_ids[0], per_coarse)
    coarse_in = (col_step * 3 + row_step) * per_coarse + inside
    coarse_out = (row_step * 3 + col_step) * per_coarse + inside
    basis = averaging_basis[0]

    left, right = pair(start, start, "col")
    across = jnp.concatenate([left, start, right], axis=0)
    near = spread(across.astype(BF16))

    g, gt, cs, og, basis_t, counts = call(
        prepare_kernel,
        [
            ((slots, window), BF16),
            ((window, slots), BF16),
            ((coarse_window, primals), BF16),
            ((primals, coarse_window), BF16),
            ((primals, slots), BF16),
            ((72, LANES), F32),
        ],
        positions[:, None],
        positions[None, :],
        coarse_in[:, None],
        coarse_in[None, :],
        coarse_out[:, None],
        basis,
    )
    panel = coarse_inverse.reshape(-1, coarse_inverse.shape[3])
    high, low = call(panel_kernel, [(panel.shape[::-1], BF16)] * 2, panel)

    weight = None
    for sweep in range(ITERS):
        third = 3 * own
        parts = call(
            residual_kernel,
            [((third, LANES), d) for d in (RES_A, RES_M, RES_A)],
            *near,
            g,
            gt,
            stiffness[0],
            loads[0],
        )
        if weight is None:
            def ride(part, k):
                pieces = []
                for j in range(3):
                    pieces.append(part[j * own : (j + 1) * own])
                    at = (3 * k + j) * 8
                    pieces.append(counts[at : at + 8].astype(part.dtype))
                return jnp.concatenate(pieces, axis=0)

            parts = [ride(part, k) for k, part in enumerate(parts)]
        owned = shared_by_columns(column, *parts)
        step = owned.shape[0] // 3
        residual = owned[step : step + own]
        near = spread(owned.astype(RES_H))
        if weight is None:
            blocks = [n[k * step + own : (k + 1) * step] for n in near for k in range(3)]
            shared = jnp.concatenate([wide(b) for b in blocks], axis=0)
            near = tuple(
                jnp.concatenate([n[k * step : k * step + own] for k in range(3)], axis=0) for n in near
            )
            (weight,) = call(weight_kernel, [((slots, LANES), F32)], shared, positions[:, None])
        third = 3 * per_coarse
        scaled, sent, kept = call(
            primal_kernel,
            [((slots, LANES), BF16), ((members, third, LANES), COARSE_A), ((third, LANES), F32)],
            *near,
            g,
            weight,
            basis_t,
            cs,
            scalar=column,
        )
        got = lax.all_to_all(sent, "col", 0, 0, tiled=True)
        (first,) = call(coarse_receive_kernel, [((8, third, LANES), RHS_1)], got, kept, scalar=column)
        first = from_everyone(first, inner)
        (second,) = call(fold_kernel, [((rows // 8, 10 * per_coarse, LANES), RHS_2)], first)
        second = from_everyone(second, outer)
        parts, _ = call(
            coarse_kernel,
            [((members, third, LANES), PART), ((rows * per_coarse, LANES), RHS_2)],
            second,
            high,
            low,
        )
        (local_part,) = call(local_kernel, [((slots, LANES), F32)], local_inverse[0], scaled)
        parts = lax.all_to_all(parts, "col", 0, 0, tiled=True)
        totals = wide(parts).sum(axis=0).astype(BF16)
        above, below = pair(totals, totals, "row")
        third = 3 * own
        parts = call(
            update_kernel,
            [((third, LANES), d) for d in (UPD_A, UPD_M, UPD_A)],
            above,
            totals,
            below,
            og,
            basis,
            weight,
            local_part,
            gt,
        )
        if sweep + 1 < ITERS:
            across = across + shared_by_columns(column, *parts)
            near = spread(across.astype(BF16))
        else:
            field = across[own : 2 * own] + owned_sum(*parts)
    return field, residual


def solution(mesh):
    in_specs = (
        P(("row", "col"), None, None),
        P(("row", "col"), None, None),
        P(("row", "col"), None, None),
        P(("row", "col"), None, None),
        P(("row", "col"), None),
        P(None, "col", None, "row"),
        P(("row", "col")),
        P(("row", "col"), None),
        P(("row", "col"), None),
    )
    out_specs = (P(("row", "col"), None), P(("row", "col"), None))
    return jax.shard_map(body, mesh=mesh, in_specs=in_specs, out_specs=out_specs, check_vma=False)
```

```python
import jax
import jax.numpy as jnp
from jax import lax
from jax.experimental import pallas as pl
from jax.experimental.pallas import tpu as pltpu
from jax.sharding import PartitionSpec as P

ITERS = 2
LANES = 128
F32 = jnp.float32
BF16 = jnp.bfloat16
RES_A, RES_M, RES_H = BF16, F32, F32
UPD_A, UPD_M, UPD_B = BF16, F32, F32
PART = F32


def dot(a, b):
    return jnp.dot(a, b, preferred_element_type=F32)


def call(kernel, outs, *args, scalar=None, scratch=()):
    specs = [pl.BlockSpec(memory_space=pltpu.VMEM)] * len(args)
    if scalar is not None:
        specs = [pl.BlockSpec(memory_space=pltpu.SMEM)] + specs
        args = (scalar, *args)
    return pl.pallas_call(
        kernel,
        out_shape=tuple(jax.ShapeDtypeStruct(s, d) for s, d in outs),
        in_specs=specs,
        scratch_shapes=[pltpu.VMEM(*shape) for shape in scratch],
        compiler_params=pltpu.CompilerParams(vmem_limit_bytes=48 * 1024 * 1024),
    )(*args)


def window_positions(wanted, per_owner):
    members = lax.axis_size("col")
    owner = wanted // per_owner
    row_step = owner // members - lax.axis_index("row") + 1
    col_step = owner % members - lax.axis_index("col") + 1
    return row_place(row_step), col_step, wanted % per_owner


def pair(to_far, to_near, axis):
    count = lax.axis_size(axis)
    near = [(i, i ^ 1) for i in range(count)]
    far = [(i, i - 1 + 2 * (i % 2)) for i in range(1, count - 1)]
    from_near = lax.ppermute(to_near, axis, near)
    from_far = lax.ppermute(to_far, axis, far)
    return from_near, from_far


def shifts(to_next, to_previous):
    count = lax.axis_size("col")
    from_previous = lax.ppermute(to_next, "col", [(i, i + 1) for i in range(count - 1)])
    from_next = lax.ppermute(to_previous, "col", [(i + 1, i) for i in range(count - 1)])
    return from_previous, from_next


def row_place(step):
    odd = lax.axis_index("row") % 2
    return jnp.where(odd == 0, 2 - step, step)


def from_everyone(copies, axis, groups):
    return lax.all_to_all(copies, axis, 0, 0, axis_index_groups=groups, tiled=True)


def wide(a):
    return a.astype(F32)


def spread(column):
    from_previous, from_next = pair(column, column, "row")
    return from_previous, column, from_next


def shared_by_columns(column, up, middle, down):
    from_previous, from_next = pair(down, up, "row")
    members = lax.axis_size("col")
    third = middle.shape[0] // 3
    summed, sent = call(
        send_kernel,
        [(middle.shape, F32), ((members, 2 * third, LANES), BF16)],
        from_previous,
        middle,
        from_next,
        scalar=column,
    )
    got = lax.all_to_all(sent, "col", 0, 0, tiled=True)
    (assembled,) = call(receive_kernel, [(middle.shape, F32)], got, summed, scalar=column)
    return assembled


def owned_sum(up, middle, down):
    from_previous, from_next = pair(down, up, "row")
    summed = wide(middle) + wide(from_previous) + wide(from_next)
    third = summed.shape[0] // 3
    left, own, right = summed[:third], summed[third : 2 * third], summed[2 * third :]
    from_previous, from_next = shifts(right.astype(UPD_B), left.astype(UPD_B))
    return own + wide(from_previous) + wide(from_next)


def nth(c, step, members):
    return lax.rem(c + step + members, members)


def send_kernel(column, from_previous, middle, from_next, summed, sent):
    third = middle.shape[0] // 3
    members = sent.shape[0]
    c = column[0]
    total = wide(from_previous[...]) + wide(middle[...]) + wide(from_next[...])
    summed[...] = total
    left, own, right = (total[k * third : (k + 1) * third].astype(BF16) for k in range(3))
    sent[nth(c, 1, members), :third, :] = own
    sent[nth(c, 1, members), third:, :] = right
    sent[nth(c, 2, members), :third, :] = right
    sent[nth(c, -1, members), :third, :] = own
    sent[nth(c, -1, members), third:, :] = left
    sent[nth(c, -2, members), :third, :] = left


def receive_kernel(column, got, summed, out):
    third = summed.shape[0] // 3
    members = got.shape[0]
    c = column[0]

    def part(step, rows):
        there = (c + step >= 0) & (c + step < members)
        return jnp.where(there, wide(got[nth(c, step, members), rows, :]), 0.0)

    first, second = slice(0, third), slice(third, 2 * third)
    out[:third] = summed[:third] + part(-1, first) + part(-2, first)
    out[third : 2 * third] = summed[third : 2 * third] + part(-1, second) + part(1, second)
    out[2 * third :] = summed[2 * third :] + part(1, first) + part(2, first)


def coarse_receive_kernel(place, got, kept, out):
    members = got.shape[0] // 2
    c, k = place[0], place[1]
    block = kept.shape[0] // 2
    total = kept[...]
    first = jnp.zeros((block, LANES), F32)
    for step in (-1, 0, 1):
        there = (c + step >= 0) & (c + step < members)
        at = nth(c, step, members)
        if step:
            total = total + jnp.where(there, wide(got[k * members + at]), 0.0)
        first = first + jnp.where(there, wide(got[(1 - k) * members + at, :block, :]), 0.0)
    total = total + jnp.concatenate([first, jnp.zeros((block, LANES), F32)], axis=0)
    total = total.astype(out.dtype)
    for copy in range(out.shape[0]):
        out[copy] = total


def prepare_kernel(pos_col, pos_row, coarse_col, coarse_row, out_col, basis, g, gt, cs, og, basis_t, counts):
    slots, window = g.shape
    own = window // 9
    g[...] = (pos_col[...] == lax.broadcasted_iota(jnp.int32, (slots, window), 1)).astype(F32).astype(BF16)
    gt[...] = (pos_row[...] == lax.broadcasted_iota(jnp.int32, (window, slots), 0)).astype(F32).astype(BF16)
    cs[...] = (coarse_row[...] == lax.broadcasted_iota(jnp.int32, cs.shape, 0)).astype(F32).astype(BF16)
    og[...] = (out_col[...] == lax.broadcasted_iota(jnp.int32, og.shape, 1)).astype(F32).astype(BF16)
    basis_t[...] = wide(basis[...]).T.astype(BF16)
    lane = lax.broadcasted_iota(jnp.int32, (slots, LANES), 1)
    counts[...] = jnp.zeros_like(counts)
    pos = jnp.broadcast_to(pos_col[...], (slots, LANES))
    for block in range(9):
        for half in range(-(-own // LANES)):
            hit = pos == lane + (block * own + half * LANES)
            row = block * 8 + half
            counts[row : row + 1, :] = jnp.sum(hit.astype(F32), axis=0, keepdims=True)


def panel_kernel(panel, high, low):
    turned = panel[...].T
    top = turned.astype(BF16)
    high[...] = top
    low[...] = (turned - top.astype(F32)).astype(BF16)


def picked(g, values):
    if values.dtype == BF16:
        return dot(g, values)
    high = values.astype(BF16)
    return dot(g, high) + dot(g, (values - wide(high)).astype(BF16))


def gathered(g, left, middle, right):
    third = left.shape[0]
    return (
        picked(g[:, :third], left) + picked(g[:, third : 2 * third], middle) + picked(g[:, 2 * third :], right)
    )


def scattered(gt, values, left, middle, right):
    third = left.shape[0]
    high = values.astype(BF16)
    low = (values - wide(high)).astype(BF16)
    for k, out in enumerate((left, middle, right)):
        rows = gt[k * third : (k + 1) * third]
        placed = dot(rows, high)
        if out.dtype == F32:
            placed = placed + dot(rows, low)
        out[...] = placed.astype(out.dtype)


def residual_kernel(win_l, win_m, win_r, g, gt, stiffness, loads, out_l, out_m, out_r):
    iterate = gathered(g, win_l[...], win_m[...], win_r[...]).astype(BF16)
    terms = wide(loads[...]) - dot(stiffness[...], iterate)
    scattered(gt, terms, out_l, out_m, out_r)


def weight_kernel(counts, pos_col, weight):
    slots = pos_col.shape[0]
    own = weight_own(counts)
    lane = lax.broadcasted_iota(jnp.int32, (slots, LANES), 1)
    pos = jnp.broadcast_to(pos_col[...], (slots, LANES))
    total = jnp.zeros((slots, LANES), F32)
    for block in range(9):
        for half in range(-(-own // LANES)):
            left = own - half * LANES
            hit = pos == lane + (block * own + half * LANES)
            if left < LANES:
                hit = hit & (lane < left)
            row = block * 8 + half
            total = total + jnp.where(hit, counts[row : row + 1, :], 0.0)
    shared = jnp.sum(total, axis=1, keepdims=True)
    live = (pos_col[...] >= 0).astype(F32)
    weight[...] = jnp.broadcast_to(live / (shared + 1.0 - live), weight.shape)


def weight_own(counts):
    return OWN_OF[counts.shape[0]]


OWN_OF = {}


def primal_kernel(place, up, middle, down, g, weight, basis_t, cs, scaled, sent, kept):
    rows = gathered(g, up[...], middle[...], down[...])
    values = (weight[...] * rows).astype(BF16)
    scaled[...] = values
    primal = dot(basis_t[...], values)
    block = kept.shape[0] // 2
    third = 3 * block
    members = sent.shape[0] // 2
    c, k = place[0], place[1]
    high = primal.astype(BF16)
    low = (primal - wide(high)).astype(BF16)
    for step in (-1, 0, 1):
        rows = cs[(step + 1) * third : (step + 2) * third]
        placed = dot(rows, high)
        at = nth(c, step, members)
        sent[(1 - k) * members + at, :block, :] = placed[:block].astype(BF16)
        if step:
            sent[k * members + at] = placed[block:].astype(BF16)
        else:
            kept[...] = (placed + dot(rows, low))[block:]


def local_kernel(local_inverse, scaled, out):
    out[...] = dot(local_inverse[...], scaled[...])


def coarse_kernel(halves, high, low, out, rhs):
    pairs = halves.shape[1]
    third = halves.shape[2] // 2
    for j in range(pairs):
        own = wide(halves[0, j, :third, :])
        if j > 0:
            own = own + wide(halves[1, j - 1, third:, :])
        rhs[2 * j * third : (2 * j + 1) * third, :] = own
        own = wide(halves[1, j, :third, :])
        if j + 1 < pairs:
            own = own + wide(halves[0, j + 1, third:, :])
        rhs[(2 * j + 1) * third : (2 * j + 2) * third, :] = own
    values = rhs[...]
    top = values.astype(BF16)
    rest = (values - wide(top)).astype(BF16)
    part = dot(high[...], top) + dot(low[...], top) + dot(high[...], rest)
    part = part.astype(out.dtype)
    members = out.shape[0]
    for c in range(members):
        for step in range(3):
            owner = c + step - 1
            rows = slice(step * third, (step + 1) * third)
            if 0 <= owner < members:
                out[c, rows, :] = part[owner * third : (owner + 1) * third]
            else:
                out[c, rows, :] = jnp.zeros((third, LANES), out.dtype)


def update_kernel(sol_u, sol_m, sol_d, og, basis, weight, local_part, gt, out_l, out_m, out_r):
    third = sol_u.shape[0]
    coarse = (
        dot(og[:, :third], sol_u[...])
        + dot(og[:, third : 2 * third], sol_m[...])
        + dot(og[:, 2 * third :], sol_d[...])
    ).astype(BF16)
    update = weight[...] * (local_part[...] + dot(basis[...], coarse))
    scattered(gt, update, out_l, out_m, out_r)


def body(stiffness, local_inverse, averaging_basis, loads, start, coarse_inverse, sizes, dof_ids, coarse_ids):
    own = start.shape[0]
    per_coarse = coarse_inverse.shape[2]
    slots = dof_ids.shape[1]
    primals = coarse_ids.shape[1]
    rows = lax.axis_size("row")
    members = lax.axis_size("col")
    window, coarse_window = 9 * own, 9 * per_coarse
    tiles = [[2 * members * j + m for m in range(2 * members)] for j in range(rows // 2)]
    sides = [[2 * j + k for j in range(rows // 2)] for k in range(2)]
    chips = [[2 * j, 2 * j + 1] for j in range(rows // 2)]
    OWN_OF[72] = own

    column = jnp.stack([lax.axis_index("col"), lax.axis_index("row") % 2]).astype(jnp.int32)

    active = jnp.arange(slots, dtype=jnp.int32) < sizes[0]
    row_step, col_step, inside = window_positions(dof_ids[0], own)
    positions = jnp.where(active, (row_step * 3 + col_step) * own + inside, -1)
    row_step, col_step, inside = window_positions(coarse_ids[0], per_coarse)
    coarse_in = (col_step * 3 + row_step) * per_coarse + inside
    coarse_out = (row_step * 3 + col_step) * per_coarse + inside
    basis = averaging_basis[0]

    left, right = shifts(start, start)
    across = jnp.concatenate([left, start, right], axis=0)
    near = spread(across.astype(BF16))

    g, gt, cs, og, basis_t, counts = call(
        prepare_kernel,
        [
            ((slots, window), BF16),
            ((window, slots), BF16),
            ((coarse_window, primals), BF16),
            ((primals, coarse_window), BF16),
            ((primals, slots), BF16),
            ((72, LANES), F32),
        ],
        positions[:, None],
        positions[None, :],
        coarse_in[:, None],
        coarse_in[None, :],
        coarse_out[:, None],
        basis,
    )
    panel = coarse_inverse.reshape(-1, coarse_inverse.shape[3])
    high, low = call(panel_kernel, [(panel.shape[::-1], BF16)] * 2, panel)

    weight = None
    for sweep in range(ITERS):
        third = 3 * own
        parts = call(
            residual_kernel,
            [((third, LANES), d) for d in (RES_A, RES_M, RES_A)],
            *near,
            g,
            gt,
            stiffness[0],
            loads[0],
        )
        if weight is None:
            def ride(part, k):
                pieces = []
                for j in range(3):
                    pieces.append(part[j * own : (j + 1) * own])
                    at = (3 * k + j) * 8
                    pieces.append(counts[at : at + 8].astype(part.dtype))
                return jnp.concatenate(pieces, axis=0)

            parts = [ride(part, k) for k, part in enumerate(parts)]
        owned = shared_by_columns(column, *parts)
        step = owned.shape[0] // 3
        residual = owned[step : step + own]
        near = spread(owned.astype(RES_H))
        if weight is None:
            blocks = [n[k * step + own : (k + 1) * step] for n in near for k in range(3)]
            shared = jnp.concatenate([wide(b) for b in blocks], axis=0)
            near = tuple(
                jnp.concatenate([n[k * step : k * step + own] for k in range(3)], axis=0) for n in near
            )
            (weight,) = call(weight_kernel, [((slots, LANES), F32)], shared, positions[:, None])
        scaled, sent, kept = call(
            primal_kernel,
            [
                ((slots, LANES), BF16),
                ((2 * members, 2 * per_coarse, LANES), BF16),
                ((2 * per_coarse, LANES), F32),
            ],
            *near,
            g,
            weight,
            basis_t,
            cs,
            scalar=column,
        )
        got = from_everyone(sent, ("row", "col"), tiles)
        (held,) = call(
            coarse_receive_kernel, [((rows // 2, 2 * per_coarse, LANES), BF16)], got, kept, scalar=column
        )
        side = from_everyone(held, "row", sides)
        both = from_everyone(jnp.broadcast_to(side[None], (2, *side.shape)), "row", chips)
        third = 3 * per_coarse
        (parts,) = call(
            coarse_kernel,
            [((members, third, LANES), PART)],
            both,
            high,
            low,
            scratch=[((rows * per_coarse, LANES), F32)],
        )
        (local_part,) = call(local_kernel, [((slots, LANES), F32)], local_inverse[0], scaled)
        parts = lax.all_to_all(parts, "col", 0, 0, tiled=True)
        totals = wide(parts).sum(axis=0).astype(BF16)
        above, below = pair(totals, totals, "row")
        third = 3 * own
        parts = call(
            update_kernel,
            [((third, LANES), d) for d in (UPD_A, UPD_M, UPD_A)],
            above,
            totals,
            below,
            og,
            basis,
            weight,
            local_part,
            gt,
        )
        if sweep + 1 < ITERS:
            across = across + shared_by_columns(column, *parts)
            near = spread(across.astype(BF16))
        else:
            field = across[own : 2 * own] + owned_sum(*parts)
    return field, residual


def solution(mesh):
    in_specs = (
        P(("row", "col"), None, None),
        P(("row", "col"), None, None),
        P(("row", "col"), None, None),
        P(("row", "col"), None, None),
        P(("row", "col"), None),
        P(None, "col", None, "row"),
        P(("row", "col")),
        P(("row", "col"), None),
        P(("row", "col"), None),
    )
    out_specs = (P(("row", "col"), None), P(("row", "col"), None))
    return jax.shard_map(body, mesh=mesh, in_specs=in_specs, out_specs=out_specs, check_vma=False)
```

```python
import jax
import jax.numpy as jnp
from jax import lax
from jax.experimental import pallas as pl
from jax.experimental.pallas import tpu as pltpu
from jax.sharding import PartitionSpec as P

ITERS = 2
LANES = 128
F32 = jnp.float32
BF16 = jnp.bfloat16
RES_A, RES_M = BF16, F32
UPD_A, UPD_M = BF16, F32
PART = F32


def dot(a, b):
    return jnp.dot(a, b, preferred_element_type=F32)


def call(kernel, outs, *args, scalar=None, scratch=()):
    specs = [pl.BlockSpec(memory_space=pltpu.VMEM)] * len(args)
    if scalar is not None:
        specs = [pl.BlockSpec(memory_space=pltpu.SMEM)] + specs
        args = (scalar, *args)
    return pl.pallas_call(
        kernel,
        out_shape=tuple(jax.ShapeDtypeStruct(s, d) for s, d in outs),
        in_specs=specs,
        scratch_shapes=[pltpu.VMEM(*shape) for shape in scratch],
        compiler_params=pltpu.CompilerParams(vmem_limit_bytes=48 * 1024 * 1024),
    )(*args)


def window_positions(wanted, per_owner):
    members = lax.axis_size("col")
    owner = wanted // per_owner
    row_step = owner // members - lax.axis_index("row") + 1
    col_step = owner % members - lax.axis_index("col") + 1
    return row_step, col_step, wanted % per_owner


def pair(to_far, to_near, axis):
    count = lax.axis_size(axis)
    near = [(i, i ^ 1) for i in range(count)]
    far = [(i, i - 1 + 2 * (i % 2)) for i in range(1, count - 1)]
    from_near = lax.ppermute(to_near, axis, near)
    from_far = lax.ppermute(to_far, axis, far)
    return from_near, from_far


def shifts(to_next, to_previous, axis):
    count = lax.axis_size(axis)
    from_previous = lax.ppermute(to_next, axis, [(i, i + 1) for i in range(count - 1)])
    from_next = lax.ppermute(to_previous, axis, [(i + 1, i) for i in range(count - 1)])
    return from_previous, from_next


def row_place(step):
    odd = lax.axis_index("row") % 2
    return jnp.where(odd == 0, 2 - step, step)


def from_everyone(copies, axis, groups):
    return lax.all_to_all(copies, axis, 0, 0, axis_index_groups=groups, tiled=True)


def wide(a):
    return a.astype(F32)


def spread(column):
    from_previous, from_next = shifts(column.astype(BF16), column.astype(BF16), "row")
    return from_previous, column, from_next


def shared_by_columns(column, up, middle, down):
    from_previous, from_next = shifts(down, up, "row")
    members = lax.axis_size("col")
    third = middle.shape[0] // 3
    summed, sent = call(
        send_kernel,
        [(middle.shape, F32), ((members, 2 * third, LANES), BF16)],
        from_previous,
        middle,
        from_next,
        scalar=column,
    )
    got = lax.all_to_all(sent, "col", 0, 0, tiled=True)
    (assembled,) = call(receive_kernel, [(middle.shape, F32)], got, summed, scalar=column)
    return assembled


def owned_field(across, up, middle, down):
    from_previous, from_next = shifts(down, up, "row")
    third = middle.shape[0] // 3
    left, own, right = call(sum_kernel, [((third, LANES), F32)] * 3, from_previous, middle, from_next)
    from_previous, from_next = shifts(right, left, "col")
    (field,) = call(field_kernel, [((third, LANES), F32)], across, own, from_previous, from_next)
    return field


def nth(c, step, members):
    return lax.rem(c + step + members, members)


def send_kernel(column, from_previous, middle, from_next, summed, sent):
    third = middle.shape[0] // 3
    members = sent.shape[0]
    c = column[0]
    total = wide(from_previous[...]) + wide(middle[...]) + wide(from_next[...])
    summed[...] = total
    left, own, right = (total[k * third : (k + 1) * third].astype(BF16) for k in range(3))
    sent[nth(c, 1, members), :third, :] = own
    sent[nth(c, 1, members), third:, :] = right
    sent[nth(c, 2, members), :third, :] = right
    sent[nth(c, -1, members), :third, :] = own
    sent[nth(c, -1, members), third:, :] = left
    sent[nth(c, -2, members), :third, :] = left


def sum_kernel(from_previous, middle, from_next, left, own, right):
    third = own.shape[0]
    total = wide(from_previous[...]) + middle[...] + wide(from_next[...])
    left[...], own[...], right[...] = total[:third], total[third : 2 * third], total[2 * third :]


def field_kernel(across, own, from_previous, from_next, field):
    third = own.shape[0]
    field[...] = across[third : 2 * third] + own[...] + from_previous[...] + from_next[...]


def receive_kernel(column, got, summed, out):
    third = summed.shape[0] // 3
    members = got.shape[0]
    c = column[0]

    def part(step, rows):
        there = (c + step >= 0) & (c + step < members)
        return jnp.where(there, wide(got[nth(c, step, members), rows, :]), 0.0)

    first, second = slice(0, third), slice(third, 2 * third)
    out[:third] = summed[:third] + part(-1, first) + part(-2, first)
    out[third : 2 * third] = summed[third : 2 * third] + part(-1, second) + part(1, second)
    out[2 * third :] = summed[2 * third :] + part(1, first) + part(2, first)


def coarse_receive_kernel(place, got, kept, out):
    members = got.shape[0] // 2
    c, k = place[0], place[1]
    block = kept.shape[0] // 2
    total = kept[...]
    first = jnp.zeros((block, LANES), F32)
    for step in (-1, 0, 1):
        there = (c + step >= 0) & (c + step < members)
        at = nth(c, step, members)
        if step:
            total = total + jnp.where(there, wide(got[k * members + at]), 0.0)
        first = first + jnp.where(there, wide(got[(1 - k) * members + at, :block, :]), 0.0)
    total = total + jnp.concatenate([first, jnp.zeros((block, LANES), F32)], axis=0)
    total = total.astype(out.dtype)
    for copy in range(out.shape[0]):
        out[copy] = total


def prepare_kernel(pos_col, pos_row, coarse_col, coarse_row, out_col, basis, g, gt, cs, og, basis_t, counts):
    slots, window = g.shape
    own = window // 9
    g[...] = (pos_col[...] == lax.broadcasted_iota(jnp.int32, (slots, window), 1)).astype(F32).astype(BF16)
    gt[...] = (pos_row[...] == lax.broadcasted_iota(jnp.int32, (window, slots), 0)).astype(F32).astype(BF16)
    cs[...] = (coarse_row[...] == lax.broadcasted_iota(jnp.int32, cs.shape, 0)).astype(F32).astype(BF16)
    og[...] = (out_col[...] == lax.broadcasted_iota(jnp.int32, og.shape, 1)).astype(F32).astype(BF16)
    basis_t[...] = wide(basis[...]).T.astype(BF16)
    lane = lax.broadcasted_iota(jnp.int32, (slots, LANES), 1)
    counts[...] = jnp.zeros_like(counts)
    pos = jnp.broadcast_to(pos_col[...], (slots, LANES))
    for block in range(9):
        for half in range(-(-own // LANES)):
            hit = pos == lane + (block * own + half * LANES)
            row = block * 8 + half
            counts[row : row + 1, :] = jnp.sum(hit.astype(F32), axis=0, keepdims=True)


def panel_kernel(panel, high, low):
    turned = panel[...].T
    top = turned.astype(BF16)
    high[...] = top
    low[...] = (turned - top.astype(F32)).astype(BF16)


def picked(g, values):
    if values.dtype == BF16:
        return dot(g, values)
    high = values.astype(BF16)
    return dot(g, high) + dot(g, (values - wide(high)).astype(BF16))


def gathered(g, left, middle, right):
    third = left.shape[0]
    return (
        picked(g[:, :third], left) + picked(g[:, third : 2 * third], middle) + picked(g[:, 2 * third :], right)
    )


def scattered(gt, values, left, middle, right):
    third = left.shape[0]
    high = values.astype(BF16)
    low = (values - wide(high)).astype(BF16)
    for k, out in enumerate((left, middle, right)):
        rows = gt[k * third : (k + 1) * third]
        placed = dot(rows, high)
        if out.dtype == F32:
            placed = placed + dot(rows, low)
        out[...] = placed.astype(out.dtype)


def residual_kernel(win_l, win_m, win_r, g, gt, stiffness, loads, out_l, out_m, out_r):
    iterate = gathered(g, win_l[...], win_m[...], win_r[...]).astype(BF16)
    terms = wide(loads[...]) - dot(stiffness[...], iterate)
    scattered(gt, terms, out_l, out_m, out_r)


def weight_kernel(counts, pos_col, weight):
    slots = pos_col.shape[0]
    own = weight_own(counts)
    lane = lax.broadcasted_iota(jnp.int32, (slots, LANES), 1)
    pos = jnp.broadcast_to(pos_col[...], (slots, LANES))
    total = jnp.zeros((slots, LANES), F32)
    for block in range(9):
        for half in range(-(-own // LANES)):
            left = own - half * LANES
            hit = pos == lane + (block * own + half * LANES)
            if left < LANES:
                hit = hit & (lane < left)
            row = block * 8 + half
            total = total + jnp.where(hit, counts[row : row + 1, :], 0.0)
    shared = jnp.sum(total, axis=1, keepdims=True)
    live = (pos_col[...] >= 0).astype(F32)
    weight[...] = jnp.broadcast_to(live / (shared + 1.0 - live), weight.shape)


def weight_own(counts):
    return OWN_OF[counts.shape[0]]


OWN_OF = {}


def primal_kernel(place, up, middle, down, g, weight, basis_t, cs, scaled, sent, kept):
    rows = gathered(g, up[...], middle[...], down[...])
    values = (weight[...] * rows).astype(BF16)
    scaled[...] = values
    primal = dot(basis_t[...], values)
    block = kept.shape[0] // 2
    third = 3 * block
    members = sent.shape[0] // 2
    c, k = place[0], place[1]
    high = primal.astype(BF16)
    low = (primal - wide(high)).astype(BF16)
    for step in (-1, 0, 1):
        rows = cs[(step + 1) * third : (step + 2) * third]
        placed = dot(rows, high)
        at = nth(c, step, members)
        sent[(1 - k) * members + at, :block, :] = placed[:block].astype(BF16)
        if step:
            sent[k * members + at] = placed[block:].astype(BF16)
        else:
            kept[...] = (placed + dot(rows, low))[block:]


def local_kernel(local_inverse, scaled, out):
    out[...] = dot(local_inverse[...], scaled[...])


def coarse_kernel(halves, high, low, out, rhs):
    pairs = halves.shape[1]
    third = halves.shape[2] // 2
    for j in range(pairs):
        own = wide(halves[0, j, :third, :])
        if j > 0:
            own = own + wide(halves[1, j - 1, third:, :])
        rhs[2 * j * third : (2 * j + 1) * third, :] = own
        own = wide(halves[1, j, :third, :])
        if j + 1 < pairs:
            own = own + wide(halves[0, j + 1, third:, :])
        rhs[(2 * j + 1) * third : (2 * j + 2) * third, :] = own
    values = rhs[...]
    top = values.astype(BF16)
    rest = (values - wide(top)).astype(BF16)
    part = dot(high[...], top) + dot(low[...], top) + dot(high[...], rest)
    part = part.astype(out.dtype)
    members = out.shape[0]
    for c in range(members):
        for step in range(3):
            owner = c + step - 1
            rows = slice(step * third, (step + 1) * third)
            if 0 <= owner < members:
                out[c, rows, :] = part[owner * third : (owner + 1) * third]
            else:
                out[c, rows, :] = jnp.zeros((third, LANES), out.dtype)


def update_kernel(sol_u, sol_m, sol_d, og, basis, weight, local_part, gt, out_l, out_m, out_r):
    third = sol_u.shape[0]
    coarse = (
        dot(og[:, :third], sol_u[...])
        + dot(og[:, third : 2 * third], sol_m[...])
        + dot(og[:, 2 * third :], sol_d[...])
    ).astype(BF16)
    update = weight[...] * (local_part[...] + dot(basis[...], coarse))
    scattered(gt, update, out_l, out_m, out_r)


def body(stiffness, local_inverse, averaging_basis, loads, start, coarse_inverse, sizes, dof_ids, coarse_ids):
    own = start.shape[0]
    per_coarse = coarse_inverse.shape[2]
    slots = dof_ids.shape[1]
    primals = coarse_ids.shape[1]
    rows = lax.axis_size("row")
    members = lax.axis_size("col")
    window, coarse_window = 9 * own, 9 * per_coarse
    tiles = [[2 * members * j + m for m in range(2 * members)] for j in range(rows // 2)]
    sides = [[2 * j + k for j in range(rows // 2)] for k in range(2)]
    chips = [[2 * j, 2 * j + 1] for j in range(rows // 2)]
    OWN_OF[72] = own

    column = jnp.stack([lax.axis_index("col"), lax.axis_index("row") % 2]).astype(jnp.int32)

    active = jnp.arange(slots, dtype=jnp.int32) < sizes[0]
    row_step, col_step, inside = window_positions(dof_ids[0], own)
    positions = jnp.where(active, (row_step * 3 + col_step) * own + inside, -1)
    row_step, col_step, inside = window_positions(coarse_ids[0], per_coarse)
    row_step = row_place(row_step)
    coarse_in = (col_step * 3 + row_step) * per_coarse + inside
    coarse_out = (row_step * 3 + col_step) * per_coarse + inside
    basis = averaging_basis[0]

    left, right = shifts(start, start, "col")
    across = jnp.concatenate([left, start, right], axis=0)
    near = spread(across.astype(BF16))

    g, gt, cs, og, basis_t, counts = call(
        prepare_kernel,
        [
            ((slots, window), BF16),
            ((window, slots), BF16),
            ((coarse_window, primals), BF16),
            ((primals, coarse_window), BF16),
            ((primals, slots), BF16),
            ((72, LANES), F32),
        ],
        positions[:, None],
        positions[None, :],
        coarse_in[:, None],
        coarse_in[None, :],
        coarse_out[:, None],
        basis,
    )
    panel = coarse_inverse.reshape(-1, coarse_inverse.shape[3])
    high, low = call(panel_kernel, [(panel.shape[::-1], BF16)] * 2, panel)

    weight = None
    for sweep in range(ITERS):
        third = 3 * own
        parts = call(
            residual_kernel,
            [((third, LANES), d) for d in (RES_A, RES_M, RES_A)],
            *near,
            g,
            gt,
            stiffness[0],
            loads[0],
        )
        if weight is None:
            def ride(part, k):
                pieces = []
                for j in range(3):
                    pieces.append(part[j * own : (j + 1) * own])
                    at = (3 * k + j) * 8
                    pieces.append(counts[at : at + 8].astype(part.dtype))
                return jnp.concatenate(pieces, axis=0)

            parts = [ride(part, k) for k, part in enumerate(parts)]
        owned = shared_by_columns(column, *parts)
        step = owned.shape[0] // 3
        residual = owned[step : step + own]
        near = spread(owned)
        if weight is None:
            blocks = [n[k * step + own : (k + 1) * step] for n in near for k in range(3)]
            shared = jnp.concatenate([wide(b) for b in blocks], axis=0)
            near = tuple(
                jnp.concatenate([n[k * step : k * step + own] for k in range(3)], axis=0) for n in near
            )
            (weight,) = call(weight_kernel, [((slots, LANES), F32)], shared, positions[:, None])
        scaled, sent, kept = call(
            primal_kernel,
            [
                ((slots, LANES), BF16),
                ((2 * members, 2 * per_coarse, LANES), BF16),
                ((2 * per_coarse, LANES), F32),
            ],
            *near,
            g,
            weight,
            basis_t,
            cs,
            scalar=column,
        )
        got = from_everyone(sent, ("row", "col"), tiles)
        (held,) = call(
            coarse_receive_kernel, [((rows // 2, 2 * per_coarse, LANES), BF16)], got, kept, scalar=column
        )
        side = from_everyone(held, "row", sides)
        both = from_everyone(jnp.broadcast_to(side[None], (2, *side.shape)), "row", chips)
        third = 3 * per_coarse
        (parts,) = call(
            coarse_kernel,
            [((members, third, LANES), PART)],
            both,
            high,
            low,
            scratch=[((rows * per_coarse, LANES), F32)],
        )
        (local_part,) = call(local_kernel, [((slots, LANES), F32)], local_inverse[0], scaled)
        parts = lax.all_to_all(parts, "col", 0, 0, tiled=True)
        totals = wide(parts).sum(axis=0).astype(BF16)
        above, below = pair(totals, totals, "row")
        third = 3 * own
        parts = call(
            update_kernel,
            [((third, LANES), d) for d in (UPD_A, UPD_M, UPD_A)],
            above,
            totals,
            below,
            og,
            basis,
            weight,
            local_part,
            gt,
        )
        if sweep + 1 < ITERS:
            across = across + shared_by_columns(column, *parts)
            near = spread(across.astype(BF16))
        else:
            field = owned_field(across, *parts)
    return field, residual


def solution(mesh):
    in_specs = (
        P(("row", "col"), None, None),
        P(("row", "col"), None, None),
        P(("row", "col"), None, None),
        P(("row", "col"), None, None),
        P(("row", "col"), None),
        P(None, "col", None, "row"),
        P(("row", "col")),
        P(("row", "col"), None),
        P(("row", "col"), None),
    )
    out_specs = (P(("row", "col"), None), P(("row", "col"), None))
    return jax.shard_map(body, mesh=mesh, in_specs=in_specs, out_specs=out_specs, check_vma=False)
```

```python
import jax
import jax.numpy as jnp
from jax import lax
from jax.experimental import pallas as pl
from jax.experimental.pallas import tpu as pltpu
from jax.sharding import PartitionSpec as P

ITERS = 2
LANES = 128
F32 = jnp.float32
BF16 = jnp.bfloat16
RES_A, RES_M = BF16, F32
UPD_A, UPD_M = BF16, F32
PART = F32


def dot(a, b):
    return jnp.dot(a, b, preferred_element_type=F32)


def call(kernel, outs, *args, scalar=None, scratch=()):
    specs = [pl.BlockSpec(memory_space=pltpu.VMEM)] * len(args)
    if scalar is not None:
        specs = [pl.BlockSpec(memory_space=pltpu.SMEM)] + specs
        args = (scalar, *args)
    return pl.pallas_call(
        kernel,
        out_shape=tuple(jax.ShapeDtypeStruct(s, d) for s, d in outs),
        in_specs=specs,
        scratch_shapes=[pltpu.VMEM(*shape) for shape in scratch],
        compiler_params=pltpu.CompilerParams(vmem_limit_bytes=48 * 1024 * 1024),
    )(*args)


def window_positions(wanted, per_owner):
    members = lax.axis_size("col")
    owner = wanted // per_owner
    row_step = owner // members - lax.axis_index("row") + 1
    col_step = owner % members - lax.axis_index("col") + 1
    return row_step, col_step, wanted % per_owner


def far_swaps(count):
    return [(i, i - 1 + 2 * (i % 2)) for i in range(1, count - 1)]


def pair(to_far, to_near, axis):
    count = lax.axis_size(axis)
    near = [(i, i ^ 1) for i in range(count)]
    from_near = lax.ppermute(to_near, axis, near)
    from_far = lax.ppermute(to_far, axis, far_swaps(count))
    return from_near, from_far


def shifts(to_next, to_previous, axis):
    count = lax.axis_size(axis)
    from_previous = lax.ppermute(to_next, axis, [(i, i + 1) for i in range(count - 1)])
    from_next = lax.ppermute(to_previous, axis, [(i + 1, i) for i in range(count - 1)])
    return from_previous, from_next


def row_place(step):
    odd = lax.axis_index("row") % 2
    return jnp.where(odd == 0, 2 - step, step)


def from_everyone(copies, axis, groups):
    return lax.all_to_all(copies, axis, 0, 0, axis_index_groups=groups, tiled=True)


def wide(a):
    return a.astype(F32)


def spread(column):
    from_previous, from_next = shifts(column.astype(BF16), column.astype(BF16), "row")
    return from_previous, column, from_next


def shared_by_columns(column, up, middle, down):
    from_previous, from_next = shifts(down, up, "row")
    members = lax.axis_size("col")
    third = middle.shape[0] // 3
    summed, sent = call(
        send_kernel,
        [(middle.shape, F32), ((members, 2 * third, LANES), BF16)],
        from_previous,
        middle,
        from_next,
        scalar=column,
    )
    got = lax.all_to_all(sent, "col", 0, 0, tiled=True)
    (assembled,) = call(receive_kernel, [(middle.shape, F32)], got, summed, scalar=column)
    return assembled


def owned_field(across, up, middle, down):
    from_previous, from_next = shifts(down, up, "row")
    third = middle.shape[0] // 3
    left, own, right = call(sum_kernel, [((third, LANES), F32)] * 3, from_previous, middle, from_next)
    from_previous, from_next = shifts(right, left, "col")
    (field,) = call(field_kernel, [((third, LANES), F32)], across, own, from_previous, from_next)
    return field


def nth(c, step, members):
    return lax.rem(c + step + members, members)


def send_kernel(column, from_previous, middle, from_next, summed, sent):
    third = middle.shape[0] // 3
    members = sent.shape[0]
    c = column[0]
    total = wide(from_previous[...]) + wide(middle[...]) + wide(from_next[...])
    summed[...] = total
    left, own, right = (total[k * third : (k + 1) * third].astype(BF16) for k in range(3))
    sent[nth(c, 1, members), :third, :] = own
    sent[nth(c, 1, members), third:, :] = right
    sent[nth(c, 2, members), :third, :] = right
    sent[nth(c, -1, members), :third, :] = own
    sent[nth(c, -1, members), third:, :] = left
    sent[nth(c, -2, members), :third, :] = left


def sum_kernel(from_previous, middle, from_next, left, own, right):
    third = own.shape[0]
    total = wide(from_previous[...]) + middle[...] + wide(from_next[...])
    left[...], own[...], right[...] = total[:third], total[third : 2 * third], total[2 * third :]


def field_kernel(across, own, from_previous, from_next, field):
    third = own.shape[0]
    field[...] = across[third : 2 * third] + own[...] + from_previous[...] + from_next[...]


def receive_kernel(column, got, summed, out):
    third = summed.shape[0] // 3
    members = got.shape[0]
    c = column[0]

    def part(step, rows):
        there = (c + step >= 0) & (c + step < members)
        return jnp.where(there, wide(got[nth(c, step, members), rows, :]), 0.0)

    first, second = slice(0, third), slice(third, 2 * third)
    out[:third] = summed[:third] + part(-1, first) + part(-2, first)
    out[third : 2 * third] = summed[third : 2 * third] + part(-1, second) + part(1, second)
    out[2 * third :] = summed[2 * third :] + part(1, first) + part(2, first)


def coarse_receive_kernel(place, got, kept, own, far):
    members = got.shape[0] // 2
    c, k = place[0], place[1]
    block = kept.shape[0] // 2
    total = kept[...]
    first = jnp.zeros((block, LANES), F32)
    for step in (-1, 0, 1):
        there = (c + step >= 0) & (c + step < members)
        at = nth(c, step, members)
        if step:
            total = total + jnp.where(there, wide(got[k * members + at]), 0.0)
        first = first + jnp.where(there, wide(got[(1 - k) * members + at, :block, :]), 0.0)
    own[...] = total[:block] + first
    far[...] = total[block:].astype(far.dtype)


def coarse_copies_kernel(own, from_far, out):
    total = (own[...] + wide(from_far[...])).astype(out.dtype)
    for copy in range(out.shape[0]):
        out[copy] = total


def prepare_kernel(pos_col, pos_row, coarse_col, coarse_row, out_col, basis, g, gt, cs, og, basis_t, counts):
    slots, window = g.shape
    own = window // 9
    g[...] = (pos_col[...] == lax.broadcasted_iota(jnp.int32, (slots, window), 1)).astype(F32).astype(BF16)
    gt[...] = (pos_row[...] == lax.broadcasted_iota(jnp.int32, (window, slots), 0)).astype(F32).astype(BF16)
    cs[...] = (coarse_row[...] == lax.broadcasted_iota(jnp.int32, cs.shape, 0)).astype(F32).astype(BF16)
    og[...] = (out_col[...] == lax.broadcasted_iota(jnp.int32, og.shape, 1)).astype(F32).astype(BF16)
    basis_t[...] = wide(basis[...]).T.astype(BF16)
    lane = lax.broadcasted_iota(jnp.int32, (slots, LANES), 1)
    counts[...] = jnp.zeros_like(counts)
    pos = jnp.broadcast_to(pos_col[...], (slots, LANES))
    for block in range(9):
        for half in range(-(-own // LANES)):
            hit = pos == lane + (block * own + half * LANES)
            row = block * 8 + half
            counts[row : row + 1, :] = jnp.sum(hit.astype(F32), axis=0, keepdims=True)


def panel_kernel(panel, high, low):
    turned = panel[...].T
    top = turned.astype(BF16)
    high[...] = top
    low[...] = (turned - top.astype(F32)).astype(BF16)


def picked(g, values):
    if values.dtype == BF16:
        return dot(g, values)
    high = values.astype(BF16)
    return dot(g, high) + dot(g, (values - wide(high)).astype(BF16))


def gathered(g, left, middle, right):
    third = left.shape[0]
    return (
        picked(g[:, :third], left) + picked(g[:, third : 2 * third], middle) + picked(g[:, 2 * third :], right)
    )


def scattered(gt, values, left, middle, right):
    third = left.shape[0]
    high = values.astype(BF16)
    low = (values - wide(high)).astype(BF16)
    for k, out in enumerate((left, middle, right)):
        rows = gt[k * third : (k + 1) * third]
        placed = dot(rows, high)
        if out.dtype == F32:
            placed = placed + dot(rows, low)
        out[...] = placed.astype(out.dtype)


def residual_kernel(win_l, win_m, win_r, g, gt, stiffness, loads, out_l, out_m, out_r):
    iterate = gathered(g, win_l[...], win_m[...], win_r[...]).astype(BF16)
    terms = wide(loads[...]) - dot(stiffness[...], iterate)
    scattered(gt, terms, out_l, out_m, out_r)


def weight_kernel(counts, pos_col, weight):
    slots = pos_col.shape[0]
    own = weight_own(counts)
    lane = lax.broadcasted_iota(jnp.int32, (slots, LANES), 1)
    pos = jnp.broadcast_to(pos_col[...], (slots, LANES))
    total = jnp.zeros((slots, LANES), F32)
    for block in range(9):
        for half in range(-(-own // LANES)):
            left = own - half * LANES
            hit = pos == lane + (block * own + half * LANES)
            if left < LANES:
                hit = hit & (lane < left)
            row = block * 8 + half
            total = total + jnp.where(hit, counts[row : row + 1, :], 0.0)
    shared = jnp.sum(total, axis=1, keepdims=True)
    live = (pos_col[...] >= 0).astype(F32)
    weight[...] = jnp.broadcast_to(live / (shared + 1.0 - live), weight.shape)


def weight_own(counts):
    return OWN_OF[counts.shape[0]]


OWN_OF = {}


def primal_kernel(place, up, middle, down, g, weight, basis_t, cs, scaled, sent, kept):
    rows = gathered(g, up[...], middle[...], down[...])
    values = (weight[...] * rows).astype(BF16)
    scaled[...] = values
    primal = dot(basis_t[...], values)
    block = kept.shape[0] // 2
    third = 3 * block
    members = sent.shape[0] // 2
    c, k = place[0], place[1]
    high = primal.astype(BF16)
    low = (primal - wide(high)).astype(BF16)
    for step in (-1, 0, 1):
        rows = cs[(step + 1) * third : (step + 2) * third]
        placed = dot(rows, high)
        at = nth(c, step, members)
        sent[(1 - k) * members + at, :block, :] = placed[:block].astype(BF16)
        if step:
            sent[k * members + at] = placed[block:].astype(BF16)
        else:
            kept[...] = (placed + dot(rows, low))[block:]


def local_kernel(local_inverse, scaled, out):
    out[...] = dot(local_inverse[...], scaled[...])


def coarse_kernel(halves, high, low, out, rhs):
    pairs = halves.shape[1]
    third = halves.shape[2]
    for j in range(pairs):
        for k in range(2):
            row = 2 * j + k
            rhs[row * third : (row + 1) * third, :] = halves[k, j]
    values = rhs[...]
    part = dot(high[...], values) + dot(low[...], values)
    part = part.astype(out.dtype)
    members = out.shape[0]
    for c in range(members):
        for step in range(3):
            owner = c + step - 1
            rows = slice(step * third, (step + 1) * third)
            if 0 <= owner < members:
                out[c, rows, :] = part[owner * third : (owner + 1) * third]
            else:
                out[c, rows, :] = jnp.zeros((third, LANES), out.dtype)


def update_kernel(sol_u, sol_m, sol_d, og, basis, weight, local_part, gt, out_l, out_m, out_r):
    third = sol_u.shape[0]
    coarse = (
        dot(og[:, :third], sol_u[...])
        + dot(og[:, third : 2 * third], sol_m[...])
        + dot(og[:, 2 * third :], sol_d[...])
    ).astype(BF16)
    update = weight[...] * (local_part[...] + dot(basis[...], coarse))
    scattered(gt, update, out_l, out_m, out_r)


def body(stiffness, local_inverse, averaging_basis, loads, start, coarse_inverse, sizes, dof_ids, coarse_ids):
    own = start.shape[0]
    per_coarse = coarse_inverse.shape[2]
    slots = dof_ids.shape[1]
    primals = coarse_ids.shape[1]
    rows = lax.axis_size("row")
    members = lax.axis_size("col")
    window, coarse_window = 9 * own, 9 * per_coarse
    tiles = [[2 * members * j + m for m in range(2 * members)] for j in range(rows // 2)]
    sides = [[2 * j + k for j in range(rows // 2)] for k in range(2)]
    chips = [[2 * j, 2 * j + 1] for j in range(rows // 2)]
    OWN_OF[72] = own

    column = jnp.stack([lax.axis_index("col"), lax.axis_index("row") % 2]).astype(jnp.int32)

    active = jnp.arange(slots, dtype=jnp.int32) < sizes[0]
    row_step, col_step, inside = window_positions(dof_ids[0], own)
    positions = jnp.where(active, (row_step * 3 + col_step) * own + inside, -1)
    row_step, col_step, inside = window_positions(coarse_ids[0], per_coarse)
    row_step = row_place(row_step)
    coarse_in = (col_step * 3 + row_step) * per_coarse + inside
    coarse_out = (row_step * 3 + col_step) * per_coarse + inside
    basis = averaging_basis[0]

    left, right = shifts(start, start, "col")
    across = jnp.concatenate([left, start, right], axis=0)
    near = spread(across.astype(BF16))

    g, gt, cs, og, basis_t, counts = call(
        prepare_kernel,
        [
            ((slots, window), BF16),
            ((window, slots), BF16),
            ((coarse_window, primals), BF16),
            ((primals, coarse_window), BF16),
            ((primals, slots), BF16),
            ((72, LANES), F32),
        ],
        positions[:, None],
        positions[None, :],
        coarse_in[:, None],
        coarse_in[None, :],
        coarse_out[:, None],
        basis,
    )
    panel = coarse_inverse.reshape(-1, coarse_inverse.shape[3])
    high, low = call(panel_kernel, [(panel.shape[::-1], BF16)] * 2, panel)

    weight = None
    for sweep in range(ITERS):
        third = 3 * own
        parts = call(
            residual_kernel,
            [((third, LANES), d) for d in (RES_A, RES_M, RES_A)],
            *near,
            g,
            gt,
            stiffness[0],
            loads[0],
        )
        if weight is None:
            def ride(part, k):
                pieces = []
                for j in range(3):
                    pieces.append(part[j * own : (j + 1) * own])
                    at = (3 * k + j) * 8
                    pieces.append(counts[at : at + 8].astype(part.dtype))
                return jnp.concatenate(pieces, axis=0)

            parts = [ride(part, k) for k, part in enumerate(parts)]
        owned = shared_by_columns(column, *parts)
        step = owned.shape[0] // 3
        residual = owned[step : step + own]
        near = spread(owned)
        if weight is None:
            blocks = [n[k * step + own : (k + 1) * step] for n in near for k in range(3)]
            shared = jnp.concatenate([wide(b) for b in blocks], axis=0)
            near = tuple(
                jnp.concatenate([n[k * step : k * step + own] for k in range(3)], axis=0) for n in near
            )
            (weight,) = call(weight_kernel, [((slots, LANES), F32)], shared, positions[:, None])
        scaled, sent, kept = call(
            primal_kernel,
            [
                ((slots, LANES), BF16),
                ((2 * members, 2 * per_coarse, LANES), BF16),
                ((2 * per_coarse, LANES), F32),
            ],
            *near,
            g,
            weight,
            basis_t,
            cs,
            scalar=column,
        )
        got = from_everyone(sent, ("row", "col"), tiles)
        mine, far = call(
            coarse_receive_kernel,
            [((per_coarse, LANES), F32), ((per_coarse, LANES), BF16)],
            got,
            kept,
            scalar=column,
        )
        from_far = lax.ppermute(far, "row", far_swaps(rows))
        (held,) = call(coarse_copies_kernel, [((rows // 2, per_coarse, LANES), BF16)], mine, from_far)
        side = from_everyone(held, "row", sides)
        both = from_everyone(jnp.broadcast_to(side[None], (2, *side.shape)), "row", chips)
        third = 3 * per_coarse
        (parts,) = call(
            coarse_kernel,
            [((members, third, LANES), PART)],
            both,
            high,
            low,
            scratch=[((rows * per_coarse, LANES), BF16)],
        )
        (local_part,) = call(local_kernel, [((slots, LANES), F32)], local_inverse[0], scaled)
        parts = lax.all_to_all(parts, "col", 0, 0, tiled=True)
        totals = wide(parts).sum(axis=0).astype(BF16)
        above, below = pair(totals, totals, "row")
        third = 3 * own
        parts = call(
            update_kernel,
            [((third, LANES), d) for d in (UPD_A, UPD_M, UPD_A)],
            above,
            totals,
            below,
            og,
            basis,
            weight,
            local_part,
            gt,
        )
        if sweep + 1 < ITERS:
            across = across + shared_by_columns(column, *parts)
            near = spread(across.astype(BF16))
        else:
            field = owned_field(across, *parts)
    return field, residual


def solution(mesh):
    in_specs = (
        P(("row", "col"), None, None),
        P(("row", "col"), None, None),
        P(("row", "col"), None, None),
        P(("row", "col"), None, None),
        P(("row", "col"), None),
        P(None, "col", None, "row"),
        P(("row", "col")),
        P(("row", "col"), None),
        P(("row", "col"), None),
    )
    out_specs = (P(("row", "col"), None), P(("row", "col"), None))
    return jax.shard_map(body, mesh=mesh, in_specs=in_specs, out_specs=out_specs, check_vma=False)
```
